128 devices in a mesh: row: 8 (over x, core), col: 4 (over z), depth: 4 (over y).
Axes of the slice: x: 4, y: 4, z: 4, core: 2. Of those that a mesh axis runs over, the one named last changes fastest.
Arguments:
- trailing: float32 [8192, 8192], P('row', 'col'), may hold values from -6 to 6
- panel: bfloat16 [8192, 4096], P('row', 'col'), may hold values from -0.75 to 0.75
- inverse_factor: bfloat16 [4096, 4096], P('depth', 'col'), may hold values from -0.09375 to 0.09375
- block_inverse: float32 [8192, 512], P('row'), may hold values from -0.25 to 0.25
- guess: float32 [8192, 128], P(('col', 'depth')), may hold values from -0.0625 to 0.0625
- target: float32 [8192, 128], P('row'), may hold values from -6 to 6
Outputs:
- updated: float32 [8192, 8192], P('row', ('col', 'depth'))
- correction: float32 [8192, 128], P('row')
- residual_rms: float32 [1], replicated
The draws below stay inside these ranges and needn't reach their ends.
All inputs are finite; a program needn't handle non-finite values.
Results may differ from the reference program's by a relative error of at most 0.00036.
Values may be sent and summed in bfloat16 or wider, within the bound.
No kernel may reach another device: no remote copies, remote signals or barrier semaphores. Data moves between devices by JAX's collectives and lax.ppermute only.
A program may use at most 128 MiB of HBM per device.

```python
import jax
import jax.numpy as jnp
from jax import lax

N = 8192
B = 4096
BS = 512
R = 128


def levels(rng, extent, cuts, smallest, high):
    def one(position, parts):
        steps = jax.random.uniform(jax.random.fold_in(jax.random.fold_in(rng, 6), position), (parts,), jnp.float32, smallest / len(cuts), high / len(cuts))
        return jnp.repeat(jnp.exp(steps), extent[position] // parts).reshape((-1,) + (1,) * (len(extent) - position - 1))

    gain = one(*cuts[0])
    for cut in cuts[1:]:
        gain = gain * one(*cut)
    return gain


def scatter_about(own_key, shape, spread, limit, shards=(), held_as=jnp.bfloat16):
    values = spread * jax.random.normal(own_key, shape, jnp.float32)
    if shards:
        values = values * levels(own_key, shape, shards, -0.22, 0.18)
    return jnp.clip(values, -limit, limit).astype(held_as)


def setup_inputs(seed: int = 0) -> dict:
    streams_of = jax.random.split(jax.random.key(seed), 7)
    trailing = scatter_about(streams_of[0], (N, N), 1.0, 6.0, ((0, 8), (1, 4)), jnp.float32)
    panel = scatter_about(streams_of[1], (N, B), 0.125, 0.75, ((0, 8), (1, 4)))
    inverse_factor = scatter_about(streams_of[2], (B, B), B ** -0.5, 0.09375, ((0, 4), (1, 4)))
    block_inverse = scatter_about(streams_of[3], (N, BS), BS ** -0.5, 0.25, ((0, 8),), jnp.float32)
    guess = scatter_about(streams_of[4], (N, R), N ** -0.5, 0.0625, ((0, 16),), jnp.float32)
    target = scatter_about(streams_of[5], (N, R), 1.0, 6.0, ((0, 8),), jnp.float32)
    return {"trailing": trailing, "panel": panel, "inverse_factor": inverse_factor, "block_inverse": block_inverse, "guess": guess, "target": target}


def reference(trailing, panel, inverse_factor, block_inverse, guess, target):
    lower = jnp.tril(inverse_factor)
    factor = jnp.dot(panel, lower.T, preferred_element_type=jnp.float32).astype(jnp.bfloat16)
    product = jnp.dot(factor, factor.T, preferred_element_type=jnp.float32)
    updated = trailing - product
    applied = jnp.dot(updated, guess, precision=lax.Precision.HIGHEST, preferred_element_type=jnp.float32)
    residual = target - applied
    residual_rms = jnp.sqrt(jnp.sum(residual * residual) / (N * R))
    blocks = jnp.tril(block_inverse.reshape(N // BS, BS, BS))
    pieces = residual.reshape(N // BS, BS, R)
    first = jnp.einsum('bij,bjr->bir', blocks, pieces, precision=lax.Precision.HIGHEST)
    second = jnp.einsum('bji,bjr->bir', blocks, first, precision=lax.Precision.HIGHEST)
    correction = second.reshape(N, R)
    return (updated, correction, residual_rms.reshape(1))
```

```python
import jax
import jax.numpy as jnp
from jax import lax
from jax.experimental import pallas as pl
from jax.experimental.pallas import tpu as pltpu
from jax.sharding import PartitionSpec as P

N = 8192
BS = 512
R = 128
F32 = jnp.float32
BF16 = jnp.bfloat16
PLANE = ("col", "depth")
ALL = ("row", "col", "depth")


def ring(size, step):
    return [(i, (i + step) % size) for i in range(size)]


def gather_ring(block, axis, step, size):
    half = block.shape[0] // 2
    prev = lax.ppermute(block, axis, ring(size, step))
    succ = lax.ppermute(block, axis, ring(size, -step))
    far_a = lax.ppermute(prev[:half], axis, ring(size, step))
    far_b = lax.ppermute(succ[half:], axis, ring(size, -step))
    return block, prev, succ, far_a, far_b


def joined(parts):
    return jnp.concatenate(parts, axis=0)


def dot_t(a, b):
    return lax.dot_general(a, b, (((1,), (1,)), ((), ())), preferred_element_type=F32)


def factor_share(panel, lower, col_id):
    def chunk(k):
        rows = lax.dynamic_slice_in_dim(panel, ((col_id + k) % 4) * 256, 256, 0)
        return dot_t(rows, lower)

    far = chunk(2)
    far_a = lax.ppermute(far[:128], "col", ring(4, 1))
    far_b = lax.ppermute(far[128:], "col", ring(4, -1))
    succ, prev, own = chunk(1), chunk(3), chunk(0)
    s_b = lax.ppermute(succ[128:], "col", ring(4, 1))
    p_a = lax.ppermute(prev[:128], "col", ring(4, -1))
    s_a = lax.ppermute(succ[:128] + far_a, "col", ring(4, 1))
    p_b = lax.ppermute(prev[128:] + far_b, "col", ring(4, -1))
    top = own[:128] + s_a + p_a
    bottom = own[128:] + s_b + p_b
    return top.astype(BF16), bottom.astype(BF16)


def turned():
    pairs = []
    for r in range(8):
        for c in range(4):
            for d in range(4):
                x, core = divmod(r, 2)
                depth = 2 * core + c // 2
                row = 2 * ((d + 2 * core + x) % 4) + c % 2
                pairs.append(((r * 4 + c) * 4 + d, (row * 4 + x) * 4 + depth))
    return pairs


def early_kernel(idx, zd, zr, zl, yd, yr, yl, bo, bx, mine, acc):
    for h, b in ((0, bo), (1, bx)):
        cols = pl.ds(pl.multiple_of(idx[8 + h] * 256, 256), 256)
        total = None
        for t, z in enumerate((zd, zr, zl, None)):
            blk = slice(128 * t, 128 * t + 128)
            parts = [yd[blk, :], yr[blk, :], yl[blk, :]]
            if z is not None:
                parts.append(z[...])
            part = dot_t(jnp.concatenate(parts, axis=0), b[idx[4 + t]])
            if total is None:
                total = part
            elif z is not None:
                total = total + part
            else:
                total = jnp.concatenate([total[:384] + part, total[384:]], axis=0)
        for i in range(3):
            rows = pl.ds(pl.multiple_of(idx[i] + 128, 128), 128)
            acc[rows, cols] = mine[rows, cols] - total[128 * i : 128 * i + 128]
        for i in range(4):
            rows = pl.ds(pl.multiple_of(idx[i], 128), 128)
            acc[rows, cols] = mine[rows, cols] - total[384 + 128 * i : 512 + 128 * i]
        rows = pl.ds(pl.multiple_of(idx[3] + 128, 128), 128)
        acc[rows, cols] = mine[rows, cols]


def late_kernel(idx, za, zb, ya, yb, bo, bx, acc, guess, updated, applied):
    updated[...] = acc[...]
    for h, b in ((0, bo), (1, bx)):
        cols = pl.ds(pl.multiple_of(idx[8 + h] * 256, 256), 256)
        opposite = jnp.concatenate([za[...], zb[...], yb[128:, :]], axis=0)
        part = dot_t(opposite, b[idx[7]])
        last = part[512:] + dot_t(ya[:128, :], b[idx[4]])
        last = last + dot_t(ya[128:, :], b[idx[5]]) + dot_t(yb[:128, :], b[idx[6]])
        for i in range(4):
            rows = pl.ds(pl.multiple_of(idx[i], 128), 128)
            updated[rows, cols] = acc[rows, cols] - part[128 * i : 128 * i + 128]
        rows = pl.ds(pl.multiple_of(idx[3] + 128, 128), 128)
        updated[rows, cols] = acc[rows, cols] - last
    applied[...] = jnp.dot(
        updated[...], guess[...], precision=lax.Precision.HIGHEST, preferred_element_type=F32
    )


def on_core(kernel, outs, inputs, flops):
    size = sum(a.size * a.dtype.itemsize for a in inputs)
    vmem = pl.BlockSpec(memory_space=pltpu.VMEM)
    smem = pl.BlockSpec(memory_space=pltpu.SMEM)
    return pl.pallas_call(
        kernel,
        out_shape=outs,
        in_specs=[smem] + [vmem] * (len(inputs) - 1),
        out_specs=jax.tree.map(lambda _: vmem, outs),
        cost_estimate=pl.CostEstimate(flops=flops, bytes_accessed=size, transcendentals=0),
        compiler_params=pltpu.CompilerParams(vmem_limit_bytes=40 * 1024 * 1024),
    )(*inputs)


def body(trailing, panel, inverse_factor, block_inverse, guess, target):
    row_id = lax.axis_index("row")
    col_id = lax.axis_index("col")
    depth_id = lax.axis_index("depth")
    x_id, core_id = row_id // 2, row_id % 2
    shape = inverse_factor.shape
    k_index = depth_id * shape[0] + lax.broadcasted_iota(jnp.int32, shape, 0)
    j_index = col_id * shape[1] + lax.broadcasted_iota(jnp.int32, shape, 1)
    lower = jnp.where(k_index >= j_index, inverse_factor, jnp.zeros_like(inverse_factor))
    top, bottom = factor_share(panel, lower, col_id)

    line = lax.ppermute(joined([top, bottom]), ALL, turned())
    b_own = joined(gather_ring(line, "row", 2, 8))
    b_other = lax.ppermute(b_own, "row", [(i, i ^ 1) for i in range(8)])
    b_own, b_other = b_own.reshape(4, 256, 1024), b_other.reshape(4, 256, 1024)

    z_all = joined(gather_ring(top, "col", 1, 4))
    y_all = joined(gather_ring(bottom, "depth", 1, 4))
    zd, zr, zl, za, zb = gather_ring(z_all, "depth", 1, 4)
    yd, yr, yl, ya, yb = gather_ring(y_all, "col", 1, 4)

    offsets = [256 * ((col_id + k) % 4) for k in (0, 3, 1, 2)]
    places = []
    for k in (0, 3, 1, 2):
        dx = (depth_id + k + 2 * (depth_id // 2) + col_id - x_id) % 4
        places.append(jnp.where(dx == 0, 0, jnp.where(dx == 3, 1, dx + 1)))
    idx = jnp.stack(offsets + places + [core_id, 1 - core_id]).astype(jnp.int32)

    mine = lax.dynamic_slice_in_dim(trailing, depth_id * 512, 512, 1)
    acc = on_core(
        early_kernel,
        jax.ShapeDtypeStruct((1024, 512), F32),
        (idx, zd, zr, zl, yd, yr, yl, b_own, b_other, mine),
        2 * 512 * 1024 * (896 * 3 + 384),
    )
    updated, applied = on_core(
        late_kernel,
        (jax.ShapeDtypeStruct((1024, 512), F32), jax.ShapeDtypeStruct((1024, R), F32)),
        (idx, za, zb, ya, yb, b_own, b_other, acc, guess),
        2 * 512 * 1024 * 1024 + 2 * 6 * 1024 * 512 * 128,
    )

    pieces = lax.all_to_all(applied.reshape(16, 64, R), PLANE, 0, 0, tiled=True)
    piece_id = col_id * 4 + depth_id
    part = lax.dynamic_slice_in_dim(target, piece_id * 64, 64, 0) - pieces.sum(axis=0)
    residual = lax.all_to_all(jnp.broadcast_to(part[None], (16, 64, R)), PLANE, 0, 0, tiled=True)
    residual = residual.reshape(1024, R)
    squares = jnp.sum(residual * residual)
    squares = lax.all_to_all(jnp.broadcast_to(squares, (8, 1, 1)), "row", 0, 0, tiled=True).sum(axis=0)
    residual_rms = jnp.sqrt(squares / (N * R))
    blocks = jnp.tril(block_inverse.reshape(2, BS, BS))
    stacked = residual.reshape(2, BS, R)
    first = jnp.einsum("bij,bjr->bir", blocks, stacked, precision=lax.Precision.HIGHEST)
    second = jnp.einsum("bji,bjr->bir", blocks, first, precision=lax.Precision.HIGHEST)
    return (updated, second.reshape(1024, R), residual_rms.reshape(1))


def solution(mesh):
    placed = (
        P("row", "col"),
        P("row", "col"),
        P("depth", "col"),
        P("row", None),
        P(("col", "depth"), None),
        P("row", None),
    )
    return jax.shard_map(
        body,
        mesh=mesh,
        in_specs=placed,
        out_specs=(P("row", ("col", "depth")), P("row", None), P()),
        check_vma=False,
    )
```

```python
import jax
import jax.numpy as jnp
from jax import lax
from jax.experimental import pallas as pl
from jax.experimental.pallas import tpu as pltpu
from jax.sharding import PartitionSpec as P


N = 8192
BS = 512
R = 128
F32 = jnp.float32
BF16 = jnp.bfloat16
PLANE = ("col", "depth")
ALL = ("row", "col", "depth")


def ring(size, step):
    return [(i, (i + step) % size) for i in range(size)]


def gather_ring(block, axis, step, size):
    half = block.shape[0] // 2
    prev = lax.ppermute(block, axis, ring(size, step))
    succ = lax.ppermute(block, axis, ring(size, -step))
    far_a = lax.ppermute(prev[:half], axis, ring(size, step))
    far_b = lax.ppermute(succ[half:], axis, ring(size, -step))
    return block, prev, succ, far_a, far_b


def gather_direct(block, axis, step, size):
    prev = lax.ppermute(block, axis, ring(size, step))
    succ = lax.ppermute(block, axis, ring(size, -step))
    far = lax.ppermute(block, axis, ring(size, 2 * step))
    return block, prev, succ, far


def joined(parts):
    return jnp.concatenate(parts, axis=0)


def dot_t(a, b):
    return lax.dot_general(a, b, (((1,), (1,)), ((), ())), preferred_element_type=F32)


def first_kernel(idx, panel, inverse, lower, fb, sb, rows, raw, sems):
    copies = [
        pltpu.make_async_copy(inverse.at[256 * i : 256 * i + 256], raw.at[256 * i : 256 * i + 256], sems.at[i])
        for i in range(4)
    ]
    for i, k in enumerate((3, 2)):
        start = pl.multiple_of(idx[k] + 128, 128)
        copies.append(
            pltpu.make_async_copy(panel.at[pl.ds(start, 128)], rows.at[128 * i : 128 * i + 128], sems.at[4 + i])
        )
    for copy in copies:
        copy.start()
    for i in range(4):
        copies[i].wait()
        block = slice(256 * i, 256 * i + 256)
        shape = (256, 1024)
        k_index = idx[4] + 256 * i + lax.broadcasted_iota(jnp.int32, shape, 0)
        j_index = idx[5] + lax.broadcasted_iota(jnp.int32, shape, 1)
        lower[block, :] = jnp.where(k_index >= j_index, raw[block, :].astype(F32), 0.0).astype(BF16)
    copies[4].wait()
    copies[5].wait()
    both = dot_t(rows[...], lower[...])
    fb[...] = both[:128]
    sb[...] = both[128:]


def second_kernel(idx, panel, lower, fa, pb, pa, sa):
    far = panel[pl.ds(pl.multiple_of(idx[3], 128), 128), :]
    prev = panel[pl.ds(pl.multiple_of(idx[1], 128), 256), :]
    succ = panel[pl.ds(pl.multiple_of(idx[2], 128), 128), :]
    out = dot_t(jnp.concatenate([far, prev, succ], axis=0), lower[...])
    fa[...] = out[:128]
    pa[...] = out[128:256]
    pb[...] = out[256:384]
    sa[...] = out[384:]


def own_kernel(idx, panel, lower, top, bottom):
    out = dot_t(panel[pl.ds(pl.multiple_of(idx[0], 128), 256), :], lower[...])
    top[...] = out[:128]
    bottom[...] = out[128:]


def factor_share(panel, inverse_factor, idx):
    piece = jax.ShapeDtypeStruct((128, 1024), F32)
    square = jax.ShapeDtypeStruct((1024, 1024), BF16)
    lower, fb, sb = on_core(
        first_kernel,
        (square, piece, piece),
        (idx, panel, inverse_factor),
        2**29,
        scratch=(
            pltpu.VMEM((256, 1024), BF16),
            pltpu.VMEM((1024, 1024), BF16),
            pltpu.SemaphoreType.DMA((6,)),
        ),
        whole=2,
    )
    s_b = lax.ppermute(sb, "col", ring(4, 1))
    far_b = lax.ppermute(fb, "col", ring(4, -1))
    fa, pb, pa, sa = on_core(second_kernel, (piece,) * 4, (idx, panel, lower), 2**30)
    far_a = lax.ppermute(fa, "col", ring(4, 1))
    p_b = lax.ppermute(pb + far_b, "col", ring(4, -1))
    p_a = lax.ppermute(pa, "col", ring(4, -1))
    s_a = lax.ppermute(sa + far_a, "col", ring(4, 1))
    own_top, own_bottom = on_core(own_kernel, (piece, piece), (idx, panel, lower), 2**29)
    top = own_top + s_a + p_a
    bottom = own_bottom + s_b + p_b
    return top.astype(BF16), bottom.astype(BF16)


def turned():
    pairs = []
    for r in range(8):
        for c in range(4):
            for d in range(4):
                x, core = divmod(r, 2)
                depth = 2 * core + c // 2
                row = 2 * ((d + 2 * core + x) % 4) + c % 2
                pairs.append(((r * 4 + c) * 4 + d, (row * 4 + x) * 4 + depth))
    return pairs


def three(x):
    high = x.astype(BF16)
    rest = x - high.astype(F32)
    mid = rest.astype(BF16)
    return high, mid, (rest - mid.astype(F32)).astype(BF16)


def full_dot(a, b):
    high, mid, low = three(a)
    b_high, b_mid, b_low = three(b)
    first = jnp.dot(high, jnp.concatenate([b_high, b_mid], axis=1), preferred_element_type=F32)
    second = jnp.dot(mid, jnp.concatenate([b_high, b_mid], axis=1), preferred_element_type=F32)
    third = jnp.dot(high, b_low, preferred_element_type=F32) + jnp.dot(low, b_high, preferred_element_type=F32)
    return first[:, :R] + ((first[:, R:] + second[:, :R]) + (second[:, R:] + third))


def early_kernel(
    idx, guess, z_all, zor, zol, zr, zl, yd, yr, yl, bt, bb, ct, cb, trailing,
    acc, applied, b_all, z_in, y_in, b_in, mine, sems,
):
    b_copies = [pltpu.make_async_copy(b, b_in.at[i], sems.at[i]) for i, b in enumerate((bt, bb, ct, cb))]
    y_copies = [pltpu.make_async_copy(y, y_in.at[i], sems.at[4 + i]) for i, y in enumerate((yd, yr, yl))]
    z_copies = [
        [pltpu.make_async_copy(z_all, z_in.at[0], sems.at[7])],
        [
            pltpu.make_async_copy(zor, z_in.at[1, :128], sems.at[8]),
            pltpu.make_async_copy(zr, z_in.at[1, 128:], sems.at[9]),
        ],
        [
            pltpu.make_async_copy(zol, z_in.at[2, :128], sems.at[10]),
            pltpu.make_async_copy(zl, z_in.at[2, 128:], sems.at[11]),
        ],
    ]
    columns = pl.ds(pl.multiple_of(idx[10] * 512, 512), 512)
    last = pltpu.make_async_copy(trailing.at[:, columns], mine, sems.at[12])
    for copy in b_copies + z_copies[0] + y_copies + z_copies[1] + z_copies[2] + [last]:
        copy.start()
    for copy in b_copies:
        copy.wait()
    z_total = y_total = None
    for t in range(4):
        b = jnp.concatenate([b_in[i, idx[4 + t]] for i in range(4)], axis=0)
        b_all[512 * t : 512 * t + 512, :] = b
        if t < 3:
            for copy in z_copies[t]:
                copy.wait()
            part = dot_t(z_in[t], b)
            z_total = part if t == 0 else z_total + part
        if t == 0:
            for copy in y_copies:
                copy.wait()
        y = jnp.concatenate([y_in[i, 128 * t : 128 * t + 128, :] for i in range(3)], axis=0)
        part = dot_t(y, b)
        y_total = part if t == 0 else y_total + part
    last.wait()
    for h in range(2):
        cols = pl.ds(pl.multiple_of(idx[8 + h] * 256, 256), 256)
        half = slice(256 * h, 256 * h + 256)
        for i in range(4):
            rows = pl.ds(pl.multiple_of(idx[i], 128), 128)
            acc[rows, cols] = mine[rows, cols] - z_total[128 * i : 128 * i + 128, half]
            rows = pl.ds(pl.multiple_of(idx[i] + 128, 128), 128)
            if i < 3:
                acc[rows, cols] = mine[rows, cols] - y_total[128 * i : 128 * i + 128, half]
            else:
                acc[rows, cols] = mine[rows, cols]
    applied[...] = full_dot(acc[...], guess[...])


def late_kernel(idx, za, zb, ya, yb, b_all, acc, early, guess, updated, applied, part):
    z = jnp.concatenate([za[...], zb[...], yb[128:, :]], axis=0)
    z = dot_t(z, b_all[1536:, :])
    y = z[512:]
    for t, block in enumerate((ya[:128, :], ya[128:, :], yb[:128, :])):
        y = y + dot_t(block, b_all[512 * t : 512 * t + 512, :])
    for h in range(2):
        cols = pl.ds(pl.multiple_of(idx[8 + h] * 256, 256), 256)
        half = slice(256 * h, 256 * h + 256)
        part[:512, cols] = z[:512, half]
        part[512:, cols] = y[:, half]
    last = full_dot(part[...], guess[...])
    updated[...] = acc[...]
    applied[...] = early[...]
    for i in range(5):
        start = idx[i] if i < 4 else idx[3] + 128
        rows = pl.ds(pl.multiple_of(start, 128), 128)
        mine = slice(128 * i, 128 * i + 128)
        updated[rows, :] = acc[rows, :] - part[mine, :]
        applied[rows, :] = early[rows, :] - last[mine]


def on_core(kernel, outs, inputs, flops, vmem_mib=24, scratch=(), whole=0):
    size = sum(a.size * a.dtype.itemsize for a in inputs)
    vmem = pl.BlockSpec(memory_space=pltpu.VMEM)
    smem = pl.BlockSpec(memory_space=pltpu.SMEM)
    away = pl.BlockSpec(memory_space=pltpu.HBM)
    return pl.pallas_call(
        kernel,
        out_shape=outs,
        in_specs=[smem] + [vmem] * (len(inputs) - 1 - whole) + [away] * whole,
        out_specs=jax.tree.map(lambda _: vmem, outs),
        scratch_shapes=list(scratch),
        cost_estimate=pl.CostEstimate(flops=flops, bytes_accessed=size, transcendentals=0),
        compiler_params=pltpu.CompilerParams(vmem_limit_bytes=vmem_mib * 1024 * 1024),
    )(*inputs)


def pack_kernel(own, prev, succ, far, out):
    for i, part in enumerate((own, prev, succ, far)):
        out[i] = part[...]


def pack(parts):
    vmem = pl.BlockSpec(memory_space=pltpu.VMEM)
    return pl.pallas_call(
        pack_kernel,
        out_shape=jax.ShapeDtypeStruct((4, *parts[0].shape), parts[0].dtype),
        in_specs=[vmem] * 4,
        out_specs=vmem,
        cost_estimate=pl.CostEstimate(flops=2**20, bytes_accessed=2**22, transcendentals=0),
        compiler_params=pltpu.CompilerParams(vmem_limit_bytes=8 * 1024 * 1024),
    )(*parts)


def gram_kernel(inverse, gram):
    keep = lax.broadcasted_iota(jnp.int32, (BS, BS), 0) >= lax.broadcasted_iota(jnp.int32, (BS, BS), 1)
    for i in range(2):
        g = jnp.where(keep, inverse[BS * i : BS * i + BS, :], 0.0)
        gram[i] = lax.dot_general(
            g, g, (((0,), (0,)), ((), ())), precision=lax.Precision.HIGHEST, preferred_element_type=F32
        )


def correct_kernel(gram, residual, correction):
    for i in range(2):
        rows = slice(BS * i, BS * i + BS)
        correction[rows, :] = full_dot(gram[i], residual[rows, :])


def body(trailing, panel, inverse_factor, block_inverse, guess, target):
    row_id = lax.axis_index("row")
    col_id = lax.axis_index("col")
    depth_id = lax.axis_index("depth")
    x_id, core_id = row_id // 2, row_id % 2
    starts = [256 * ((col_id + k) % 4) for k in (0, 3, 1, 2)]
    at = jnp.stack(starts + [depth_id * 1024, col_id * 1024]).astype(jnp.int32)
    top, bottom = factor_share(panel, inverse_factor, at)

    gram = pl.pallas_call(
        gram_kernel,
        out_shape=jax.ShapeDtypeStruct((2, BS, BS), F32),
        cost_estimate=pl.CostEstimate(flops=2**32, bytes_accessed=2**22, transcendentals=0),
        compiler_params=pltpu.CompilerParams(vmem_limit_bytes=16 * 1024 * 1024),
    )(block_inverse)

    b_own, b_other = [], []
    for half in (top, bottom):
        line = lax.ppermute(half, ALL, turned())
        parts = gather_direct(line, "row", 2, 8)
        packed = pack(parts)
        b_own.append(packed)
        b_other.append(lax.ppermute(packed, "row", [(i, i ^ 1) for i in range(8)]))

    z_parts = gather_direct(top, "col", 1, 4)
    z_all = joined(z_parts)
    y_all = joined(gather_direct(bottom, "depth", 1, 4))
    z_own_r = lax.ppermute(top, "depth", ring(4, 1))
    z_own_l = lax.ppermute(top, "depth", ring(4, -1))
    z_rest = joined(z_parts[1:])
    zr = lax.ppermute(z_rest, "depth", ring(4, 1))
    zl = lax.ppermute(z_rest, "depth", ring(4, -1))
    za = lax.ppermute(joined([z_own_r, zr[:128]]), "depth", ring(4, 1))
    zb = lax.ppermute(zl[128:], "depth", ring(4, -1))
    yd, yr, yl, ya, yb = gather_ring(y_all, "col", 1, 4)

    offsets = [256 * ((col_id + k) % 4) for k in (0, 3, 1, 2)]
    places = []
    for k in (0, 3, 1, 2):
        dx = (depth_id + k + 2 * (depth_id // 2) + col_id - x_id) % 4
        places.append(jnp.where(dx == 0, 0, jnp.where(dx == 3, 1, dx + 1)))
    idx = jnp.stack(offsets + places + [core_id, 1 - core_id, depth_id]).astype(jnp.int32)

    tile = jax.ShapeDtypeStruct((1024, 512), F32)
    narrow = jax.ShapeDtypeStruct((1024, R), F32)
    acc, early, b_all = on_core(
        early_kernel,
        (tile, narrow, jax.ShapeDtypeStruct((2048, 1024), BF16)),
        (idx, guess, z_all, z_own_r, z_own_l, zr, zl, yd, yr, yl, *b_own, *b_other, trailing),
        2 * 512 * 1024 * (896 * 3 + 384),
        vmem_mib=40,
        scratch=(
            pltpu.VMEM((3, 512, 1024), BF16),
            pltpu.VMEM((3, 512, 1024), BF16),
            pltpu.VMEM((4, 4, 128, 1024), BF16),
            pltpu.VMEM((1024, 512), F32),
            pltpu.SemaphoreType.DMA((13,)),
        ),
        whole=13,
    )
    updated, applied = on_core(
        late_kernel,
        (tile, narrow),
        (idx, za, zb, ya, yb, b_all, acc, early, guess),
        2 * 512 * 1024 * 1024,
        scratch=(pltpu.VMEM((640, 512), F32),),
    )

    pieces = lax.all_to_all(applied.reshape(16, 64, R), PLANE, 0, 0, tiled=True)
    piece_id = col_id * 4 + depth_id
    part = lax.dynamic_slice_in_dim(target, piece_id * 64, 64, 0) - pieces.sum(axis=0)
    residual = lax.all_to_all(jnp.broadcast_to(part[None], (16, 64, R)), PLANE, 0, 0, tiled=True)
    residual = residual.reshape(1024, R)
    squares = jnp.sum(residual * residual)
    squares = lax.all_to_all(jnp.broadcast_to(squares, (8, 1, 1)), "row", 0, 0, tiled=True).sum(axis=0)
    residual_rms = jnp.sqrt(squares / (N * R))
    correction = pl.pallas_call(
        correct_kernel,
        out_shape=jax.ShapeDtypeStruct((1024, R), F32),
        cost_estimate=pl.CostEstimate(flops=2**30, bytes_accessed=2**22, transcendentals=0),
        compiler_params=pltpu.CompilerParams(vmem_limit_bytes=16 * 1024 * 1024),
    )(gram, residual)
    return (updated, correction, residual_rms.reshape(1))


def solution(mesh):
    placed = (
        P("row", "col"),
        P("row", "col"),
        P("depth", "col"),
        P("row", None),
        P(("col", "depth"), None),
        P("row", None),
    )
    return jax.shard_map(
        body,
        mesh=mesh,
        in_specs=placed,
        out_specs=(P("row", ("col", "depth")), P("row", None), P()),
        check_vma=False,
    )
```

```python
import jax
import jax.numpy as jnp
from jax import lax
from jax.experimental import pallas as pl
from jax.experimental.pallas import tpu as pltpu
from jax.sharding import PartitionSpec as P


N = 8192
BS = 512
R = 128
F32 = jnp.float32
BF16 = jnp.bfloat16
PLANE = ("col", "depth")
ALL = ("row", "col", "depth")


def ring(size, step):
    return [(i, (i + step) % size) for i in range(size)]


def gather_ring(block, axis, step, size):
    half = block.shape[0] // 2
    prev = lax.ppermute(block, axis, ring(size, step))
    succ = lax.ppermute(block, axis, ring(size, -step))
    cut_a, cut_b = prev[:half], succ[half:]
    far_a = lax.ppermute(cut_a, axis, ring(size, step))
    far_b = lax.ppermute(cut_b, axis, ring(size, -step))
    return block, prev, succ, far_a, far_b


def gather_direct(block, axis, step, size):
    prev = lax.ppermute(block, axis, ring(size, step))
    succ = lax.ppermute(block, axis, ring(size, -step))
    far = lax.ppermute(block, axis, ring(size, 2 * step))
    return block, prev, succ, far


def joined(parts):
    return jnp.concatenate(parts, axis=0)


def dot_t(a, b):
    return lax.dot_general(a, b, (((1,), (1,)), ((), ())), preferred_element_type=F32)


def first_kernel(idx, panel, inverse, lower, fb, sb):
    for i in range(0, 1024, 256):
        shape = (256, 1024)
        k_index = idx[4] + i + lax.broadcasted_iota(jnp.int32, shape, 0)
        j_index = idx[5] + lax.broadcasted_iota(jnp.int32, shape, 1)
        block = inverse[i : i + 256, :].astype(F32)
        lower[i : i + 256, :] = jnp.where(k_index >= j_index, block, 0.0).astype(BF16)
    far = panel[pl.ds(pl.multiple_of(idx[3] + 128, 128), 128), :]
    succ = panel[pl.ds(pl.multiple_of(idx[2] + 128, 128), 128), :]
    both = dot_t(jnp.concatenate([far, succ], axis=0), lower[...])
    fb[...] = both[:128]
    sb[...] = both[128:]


def second_kernel(idx, panel, lower, fa, pb, pa, sa):
    far = panel[pl.ds(pl.multiple_of(idx[3], 128), 128), :]
    prev = panel[pl.ds(pl.multiple_of(idx[1], 128), 256), :]
    succ = panel[pl.ds(pl.multiple_of(idx[2], 128), 128), :]
    out = dot_t(jnp.concatenate([far, prev, succ], axis=0), lower[...])
    fa[...] = out[:128]
    pa[...] = out[128:256]
    pb[...] = out[256:384]
    sa[...] = out[384:]


def own_kernel(idx, panel, lower, top, bottom):
    out = dot_t(panel[pl.ds(pl.multiple_of(idx[0], 128), 256), :], lower[...])
    top[...] = out[:128]
    bottom[...] = out[128:]


def factor_share(panel, inverse_factor, idx):
    piece = jax.ShapeDtypeStruct((128, 1024), F32)
    square = jax.ShapeDtypeStruct((1024, 1024), BF16)
    lower, fb, sb = on_core(first_kernel, (square, piece, piece), (idx, panel, inverse_factor), 2**29)
    s_b = lax.ppermute(sb, "col", ring(4, 1))
    far_b = lax.ppermute(fb, "col", ring(4, -1))
    fa, pb, pa, sa = on_core(second_kernel, (piece,) * 4, (idx, panel, lower), 2**30)
    far_a = lax.ppermute(fa, "col", ring(4, 1))
    p_b = lax.ppermute(pb + far_b, "col", ring(4, -1))
    p_a = lax.ppermute(pa, "col", ring(4, -1))
    s_a = lax.ppermute(sa + far_a, "col", ring(4, 1))
    own_top, own_bottom = on_core(own_kernel, (piece, piece), (idx, panel, lower), 2**29)
    top = own_top + s_a + p_a
    bottom = own_bottom + s_b + p_b
    return top.astype(BF16), bottom.astype(BF16)


def turned():
    pairs = []
    for r in range(8):
        for c in range(4):
            for d in range(4):
                x, core = divmod(r, 2)
                depth = 2 * core + c // 2
                row = 2 * ((d + 2 * core + x) % 4) + c % 2
                pairs.append(((r * 4 + c) * 4 + d, (row * 4 + x) * 4 + depth))
    return pairs


def three(x):
    high = x.astype(BF16)
    rest = x - high.astype(F32)
    mid = rest.astype(BF16)
    return high, mid, (rest - mid.astype(F32)).astype(BF16)


def full_dot(a, b):
    high, mid, low = three(a)
    b_high, b_mid, b_low = three(b)
    first = jnp.dot(high, jnp.concatenate([b_high, b_mid], axis=1), preferred_element_type=F32)
    second = jnp.dot(mid, jnp.concatenate([b_high, b_mid], axis=1), preferred_element_type=F32)
    third = jnp.dot(high, b_low, preferred_element_type=F32) + jnp.dot(low, b_high, preferred_element_type=F32)
    return first[:, :R] + ((first[:, R:] + second[:, :R]) + (second[:, R:] + third))


def columns_in(idx, sources, held, sems):
    return [
        [
            pltpu.make_async_copy(src.at[idx[4 + t]], held.at[t, 128 * i : 128 * i + 128], sems.at[4 * t + i])
            for i, src in enumerate(sources)
        ]
        for t in range(4)
    ]


def started(copies):
    for copy in copies:
        copy.start()


def waited(copies):
    for copy in copies:
        copy.wait()


def early_kernel(
    idx, guess, z0, z1, z2, z3, zor, zol, zr, zl, yd, yr, yl, bt, bb, ct, cb, trailing,
    acc, applied, z_in, y_in, b_in, mine, b_sems, z_sems, y_sems, sem,
):
    b_copies = columns_in(idx, (bt, bb, ct, cb), b_in, b_sems)
    place = lambda t, start, src, k: pltpu.make_async_copy(
        src, z_in.at[t, start : start + src.shape[0]], z_sems.at[k]
    )
    z_copies = [
        [place(0, 128 * i, src, i) for i, src in enumerate((z0, z1, z2, z3))],
        [place(1, 0, zor, 4), place(1, 128, zr, 5)],
        [place(2, 0, zol, 6), place(2, 128, zl, 7)],
    ]
    y_copies = [
        [
            pltpu.make_async_copy(
                src.at[128 * t : 128 * t + 128], y_in.at[t, 128 * i : 128 * i + 128], y_sems.at[3 * t + i]
            )
            for i, src in enumerate((yd, yr, yl))
        ]
        for t in range(4)
    ]
    columns = pl.ds(pl.multiple_of(idx[10] * 512, 512), 512)
    last = pltpu.make_async_copy(trailing.at[:, columns], mine, sem)
    z_copies.append([last])

    def stage(t):
        started(b_copies[t] + z_copies[t] + y_copies[t])

    stage(0)
    stage(1)
    z_total = y_total = None
    for t in range(4):
        waited(b_copies[t])
        if 1 <= t < 3:
            stage(t + 1)
        if t < 3:
            waited(z_copies[t])
            part = dot_t(z_in[t], b_in[t])
            z_total = part if t == 0 else z_total + part
        waited(y_copies[t])
        part = dot_t(y_in[t], b_in[t])
        y_total = part if t == 0 else y_total + part
    last.wait()
    for h in range(2):
        cols = pl.ds(pl.multiple_of(idx[8 + h] * 256, 256), 256)
        half = slice(256 * h, 256 * h + 256)
        for i in range(4):
            rows = pl.ds(pl.multiple_of(idx[i], 128), 128)
            acc[rows, cols] = mine[rows, cols] - z_total[128 * i : 128 * i + 128, half]
            rows = pl.ds(pl.multiple_of(idx[i] + 128, 128), 128)
            if i < 3:
                acc[rows, cols] = mine[rows, cols] - y_total[128 * i : 128 * i + 128, half]
            else:
                acc[rows, cols] = mine[rows, cols]
    applied[...] = full_dot(acc[...], guess[...])


def late_kernel(
    idx, guess, acc, early, zo, za, zb, ya, yb, bt, bb, ct, cb,
    updated, applied, z_in, y_in, b_in, part, b_sems, sems,
):
    b_copies = columns_in(idx, (bt, bb, ct, cb), b_in, b_sems)
    z_copies = [
        pltpu.make_async_copy(zo, z_in.at[:128], sems.at[0]),
        pltpu.make_async_copy(za, z_in.at[128:320], sems.at[1]),
        pltpu.make_async_copy(zb, z_in.at[320:512], sems.at[5]),
        pltpu.make_async_copy(yb.at[128:], z_in.at[512:], sems.at[2]),
    ]
    y_copies = [
        pltpu.make_async_copy(ya, y_in.at[:256], sems.at[3]),
        pltpu.make_async_copy(yb.at[:128], y_in.at[256:], sems.at[4]),
    ]
    started(b_copies[3] + z_copies + y_copies)
    for t in range(3):
        started(b_copies[t])
    waited(b_copies[3] + z_copies)
    z = dot_t(z_in[...], b_in[3])
    waited(y_copies)
    y = z[512:]
    for t in range(3):
        waited(b_copies[t])
        y = y + dot_t(y_in[128 * t : 128 * t + 128, :], b_in[t])
    for h in range(2):
        cols = pl.ds(pl.multiple_of(idx[8 + h] * 256, 256), 256)
        half = slice(256 * h, 256 * h + 256)
        part[:512, cols] = z[:512, half]
        part[512:, cols] = y[:, half]
    last = full_dot(part[...], guess[...])
    updated[...] = acc[...]
    applied[...] = early[...]
    for i in range(5):
        start = idx[i] if i < 4 else idx[3] + 128
        rows = pl.ds(pl.multiple_of(start, 128), 128)
        mine = slice(128 * i, 128 * i + 128)
        updated[rows, :] = acc[rows, :] - part[mine, :]
        applied[rows, :] = early[rows, :] - last[mine]


def on_core(kernel, outs, inputs, flops, vmem_mib=24, scratch=(), whole=0):
    size = sum(a.size * a.dtype.itemsize for a in inputs)
    vmem = pl.BlockSpec(memory_space=pltpu.VMEM)
    smem = pl.BlockSpec(memory_space=pltpu.SMEM)
    away = pl.BlockSpec(memory_space=pltpu.HBM)
    return pl.pallas_call(
        kernel,
        out_shape=outs,
        in_specs=[smem] + [vmem] * (len(inputs) - 1 - whole) + [away] * whole,
        out_specs=jax.tree.map(lambda _: vmem, outs),
        scratch_shapes=list(scratch),
        cost_estimate=pl.CostEstimate(flops=flops, bytes_accessed=size, transcendentals=0),
        compiler_params=pltpu.CompilerParams(vmem_limit_bytes=vmem_mib * 1024 * 1024),
    )(*inputs)


def pack_kernel(own, prev, succ, far, out):
    for i, part in enumerate((own, prev, succ, far)):
        out[i] = part[...]


def pack(parts):
    vmem = pl.BlockSpec(memory_space=pltpu.VMEM)
    return pl.pallas_call(
        pack_kernel,
        out_shape=jax.ShapeDtypeStruct((4, *parts[0].shape), parts[0].dtype),
        in_specs=[vmem] * 4,
        out_specs=vmem,
        cost_estimate=pl.CostEstimate(flops=2**20, bytes_accessed=2**22, transcendentals=0),
        compiler_params=pltpu.CompilerParams(vmem_limit_bytes=8 * 1024 * 1024),
    )(*parts)


def gram_kernel(inverse, gram):
    keep = lax.broadcasted_iota(jnp.int32, (BS, BS), 0) >= lax.broadcasted_iota(jnp.int32, (BS, BS), 1)
    for i in range(2):
        g = jnp.where(keep, inverse[BS * i : BS * i + BS, :], 0.0)
        gram[i] = lax.dot_general(
            g, g, (((0,), (0,)), ((), ())), precision=lax.Precision.HIGHEST, preferred_element_type=F32
        )


def correct_kernel(gram, residual, correction, squares):
    for i in range(2):
        rows = slice(BS * i, BS * i + BS)
        correction[rows, :] = full_dot(gram[i], residual[rows, :])
    total = (residual[...] * residual[...]).reshape(128, 8, R).sum(axis=0)
    squares[...] = jnp.broadcast_to(total[None], (8, 8, R))


def body(trailing, panel, inverse_factor, block_inverse, guess, target):
    row_id = lax.axis_index("row")
    col_id = lax.axis_index("col")
    depth_id = lax.axis_index("depth")
    x_id, core_id = row_id // 2, row_id % 2
    starts = [256 * ((col_id + k) % 4) for k in (0, 3, 1, 2)]
    at = jnp.stack(starts + [depth_id * 1024, col_id * 1024]).astype(jnp.int32)
    top, bottom = factor_share(panel, inverse_factor, at)

    gram = pl.pallas_call(
        gram_kernel,
        out_shape=jax.ShapeDtypeStruct((2, BS, BS), F32),
        cost_estimate=pl.CostEstimate(flops=2**32, bytes_accessed=2**22, transcendentals=0),
        compiler_params=pltpu.CompilerParams(vmem_limit_bytes=16 * 1024 * 1024),
    )(block_inverse)

    b_own, b_other = [], []
    for half in (top, bottom):
        line = lax.ppermute(half, ALL, turned())
        parts = gather_direct(line, "row", 2, 8)
        packed = pack(parts)
        b_own.append(packed)
        b_other.append(lax.ppermute(packed, "row", [(i, i ^ 1) for i in range(8)]))

    z_parts = gather_direct(top, "col", 1, 4)
    y_all = joined(gather_direct(bottom, "depth", 1, 4))
    _, z_own_r, z_own_l, z_own_far = gather_direct(top, "depth", 1, 4)
    z_rest = joined(z_parts[1:])
    _, zr, zl, za, zb = gather_ring(z_rest, "depth", 1, 4)
    yd, yr, yl, ya, yb = gather_ring(y_all, "col", 1, 4)

    offsets = [256 * ((col_id + k) % 4) for k in (0, 3, 1, 2)]
    places = []
    for k in (0, 3, 1, 2):
        dx = (depth_id + k + 2 * (depth_id // 2) + col_id - x_id) % 4
        places.append(jnp.where(dx == 0, 0, jnp.where(dx == 3, 1, dx + 1)))
    idx = jnp.stack(offsets + places + [core_id, 1 - core_id, depth_id]).astype(jnp.int32)

    tile = jax.ShapeDtypeStruct((1024, 512), F32)
    narrow = jax.ShapeDtypeStruct((1024, R), F32)
    acc, early = on_core(
        early_kernel,
        (tile, narrow),
        (idx, guess, *z_parts, z_own_r, z_own_l, zr, zl, yd, yr, yl, *b_own, *b_other, trailing),
        2 * 512 * 1024 * (896 * 3 + 384),
        vmem_mib=60,
        scratch=(
            pltpu.VMEM((3, 512, 1024), BF16),
            pltpu.VMEM((4, 384, 1024), BF16),
            pltpu.VMEM((4, 512, 1024), BF16),
            pltpu.VMEM((1024, 512), F32),
            pltpu.SemaphoreType.DMA((16,)),
            pltpu.SemaphoreType.DMA((8,)),
            pltpu.SemaphoreType.DMA((12,)),
            pltpu.SemaphoreType.DMA,
        ),
        whole=16,
    )
    updated, applied = on_core(
        late_kernel,
        (tile, narrow),
        (idx, guess, acc, early, z_own_far, za, zb, ya, yb, *b_own, *b_other),
        2 * 512 * 1024 * 1024,
        vmem_mib=60,
        scratch=(
            pltpu.VMEM((640, 1024), BF16),
            pltpu.VMEM((384, 1024), BF16),
            pltpu.VMEM((4, 512, 1024), BF16),
            pltpu.VMEM((640, 512), F32),
            pltpu.SemaphoreType.DMA((16,)),
            pltpu.SemaphoreType.DMA((6,)),
        ),
        whole=9,
    )

    pieces = lax.all_to_all(applied.reshape(16, 64, R), PLANE, 0, 0, tiled=True)
    piece_id = col_id * 4 + depth_id
    part = lax.dynamic_slice_in_dim(target, piece_id * 64, 64, 0) - pieces.sum(axis=0)
    residual = lax.all_to_all(jnp.broadcast_to(part[None], (16, 64, R)), PLANE, 0, 0, tiled=True)
    residual = residual.reshape(1024, R)
    correction, squares = pl.pallas_call(
        correct_kernel,
        out_shape=(jax.ShapeDtypeStruct((1024, R), F32), jax.ShapeDtypeStruct((8, 8, R), F32)),
        cost_estimate=pl.CostEstimate(flops=2**30, bytes_accessed=2**22, transcendentals=0),
        compiler_params=pltpu.CompilerParams(vmem_limit_bytes=16 * 1024 * 1024),
    )(gram, residual)
    squares = lax.all_to_all(squares, "row", 0, 0, tiled=True).sum()
    residual_rms = jnp.sqrt(squares / (N * R))
    return (updated, correction, residual_rms.reshape(1))


def solution(mesh):
    placed = (
        P("row", "col"),
        P("row", "col"),
        P("depth", "col"),
        P("row", None),
        P(("col", "depth"), None),
        P("row", None),
    )
    return jax.shard_map(
        body,
        mesh=mesh,
        in_specs=placed,
        out_specs=(P("row", ("col", "depth")), P("row", None), P()),
        check_vma=False,
    )
```

```python
import jax
import jax.numpy as jnp
from jax import lax
from jax.experimental import pallas as pl
from jax.experimental.pallas import tpu as pltpu
from jax.sharding import PartitionSpec as P


N = 8192
BS = 512
R = 128
F32 = jnp.float32
BF16 = jnp.bfloat16
PLANE = ("col", "depth")
ALL = ("row", "col", "depth")


def ring(size, step):
    return [(i, (i + step) % size) for i in range(size)]


def gather_ring(block, axis, step, size):
    half = block.shape[0] // 2
    prev = lax.ppermute(block, axis, ring(size, step))
    succ = lax.ppermute(block, axis, ring(size, -step))
    cut_a, cut_b = prev[:half], succ[half:]
    far_a = lax.ppermute(cut_a, axis, ring(size, step))
    far_b = lax.ppermute(cut_b, axis, ring(size, -step))
    return block, prev, succ, far_a, far_b


def gather_direct(block, axis, step, size):
    prev = lax.ppermute(block, axis, ring(size, step))
    succ = lax.ppermute(block, axis, ring(size, -step))
    far = lax.ppermute(block, axis, ring(size, 2 * step))
    return block, prev, succ, far


def joined(parts):
    return jnp.concatenate(parts, axis=0)


def dot_t(a, b):
    return lax.dot_general(a, b, (((1,), (1,)), ((), ())), preferred_element_type=F32)


def first_kernel(idx, panel, inverse, lower, fb, sb):
    for i in range(0, 1024, 256):
        shape = (256, 1024)
        k_index = idx[4] + i + lax.broadcasted_iota(jnp.int32, shape, 0)
        j_index = idx[5] + lax.broadcasted_iota(jnp.int32, shape, 1)
        block = inverse[i : i + 256, :].astype(F32)
        lower[i : i + 256, :] = jnp.where(k_index >= j_index, block, 0.0).astype(BF16)
    far = panel[pl.ds(pl.multiple_of(idx[3] + 128, 128), 128), :]
    succ = panel[pl.ds(pl.multiple_of(idx[2] + 128, 128), 128), :]
    both = dot_t(jnp.concatenate([far, succ], axis=0), lower[...])
    fb[...] = both[:128]
    sb[...] = both[128:]


def second_kernel(idx, panel, lower, fa, pb, pa, sa):
    far = panel[pl.ds(pl.multiple_of(idx[3], 128), 128), :]
    prev = panel[pl.ds(pl.multiple_of(idx[1], 128), 256), :]
    succ = panel[pl.ds(pl.multiple_of(idx[2], 128), 128), :]
    out = dot_t(jnp.concatenate([far, prev, succ], axis=0), lower[...])
    fa[...] = out[:128]
    pa[...] = out[128:256]
    pb[...] = out[256:384]
    sa[...] = out[384:]


def own_kernel(idx, panel, lower, top, bottom):
    out = dot_t(panel[pl.ds(pl.multiple_of(idx[0], 128), 256), :], lower[...])
    top[...] = out[:128]
    bottom[...] = out[128:]


def factor_share(panel, inverse_factor, idx):
    piece = jax.ShapeDtypeStruct((128, 1024), F32)
    square = jax.ShapeDtypeStruct((1024, 1024), BF16)
    lower, fb, sb = on_core(first_kernel, (square, piece, piece), (idx, panel, inverse_factor), 2**29)
    s_b = lax.ppermute(sb, "col", ring(4, 1))
    far_b = lax.ppermute(fb, "col", ring(4, -1))
    fa, pb, pa, sa = on_core(second_kernel, (piece,) * 4, (idx, panel, lower), 2**30)
    far_a = lax.ppermute(fa, "col", ring(4, 1))
    p_b = lax.ppermute(pb + far_b, "col", ring(4, -1))
    p_a = lax.ppermute(pa, "col", ring(4, -1))
    s_a = lax.ppermute(sa + far_a, "col", ring(4, 1))
    own_top, own_bottom = on_core(own_kernel, (piece, piece), (idx, panel, lower), 2**29)
    top = own_top + s_a + p_a
    bottom = own_bottom + s_b + p_b
    return top.astype(BF16), bottom.astype(BF16)


def turned():
    pairs = []
    for r in range(8):
        for c in range(4):
            for d in range(4):
                x, core = divmod(r, 2)
                depth = 2 * core + c // 2
                row = 2 * ((d + 2 * core + x) % 4) + c % 2
                pairs.append(((r * 4 + c) * 4 + d, (row * 4 + x) * 4 + depth))
    return pairs


def three(x):
    high = x.astype(BF16)
    rest = x - high.astype(F32)
    mid = rest.astype(BF16)
    return high, mid, (rest - mid.astype(F32)).astype(BF16)


def full_dot(a, b):
    high, mid, low = three(a)
    b_high, b_mid, b_low = three(b)
    first = jnp.dot(high, jnp.concatenate([b_high, b_mid], axis=1), preferred_element_type=F32)
    second = jnp.dot(mid, jnp.concatenate([b_high, b_mid], axis=1), preferred_element_type=F32)
    third = jnp.dot(high, b_low, preferred_element_type=F32) + jnp.dot(low, b_high, preferred_element_type=F32)
    return first[:, :R] + ((first[:, R:] + second[:, :R]) + (second[:, R:] + third))


def columns_in(idx, sources, held, sems):
    return [
        [
            pltpu.make_async_copy(src.at[idx[4 + t]], held.at[t, 128 * i : 128 * i + 128], sems.at[4 * t + i])
            for i, src in enumerate(sources)
        ]
        for t in range(4)
    ]


def started(copies):
    for copy in copies:
        copy.start()


def waited(copies):
    for copy in copies:
        copy.wait()


def early_kernel(
    idx, guess, z0, z1, z2, z3, zor, zol, zr, zl, yd, yr, yl, bt, bb, ct, cb, trailing,
    acc, applied, z_in, y_in, b_in, mine, b_sems, z_sems, y_sems, sem,
):
    b_copies = columns_in(idx, (bt, bb, ct, cb), b_in, b_sems)
    place = lambda t, start, src, k: pltpu.make_async_copy(
        src, z_in.at[t, start : start + src.shape[0]], z_sems.at[k]
    )
    z_copies = [
        [place(0, 128 * i, src, i) for i, src in enumerate((z0, z1, z2, z3))],
        [place(1, 0, zor, 4), place(1, 128, zr, 5)],
        [place(2, 0, zol, 6), place(2, 128, zl, 7)],
    ]
    y_copies = [
        [
            pltpu.make_async_copy(
                src.at[128 * t : 128 * t + 128], y_in.at[t, 128 * i : 128 * i + 128], y_sems.at[3 * t + i]
            )
            for i, src in enumerate((yd, yr, yl))
        ]
        for t in range(4)
    ]
    columns = pl.ds(pl.multiple_of(idx[10] * 512, 512), 512)
    last = pltpu.make_async_copy(trailing.at[:, columns], mine, sem)
    z_copies.append([last])

    def stage(t):
        started(b_copies[t] + z_copies[t] + y_copies[t])

    stage(0)
    stage(1)
    z_total = y_total = None
    for t in range(4):
        waited(b_copies[t])
        if 1 <= t < 3:
            stage(t + 1)
        if t < 3:
            waited(z_copies[t])
            part = dot_t(z_in[t], b_in[t])
            z_total = part if t == 0 else z_total + part
        waited(y_copies[t])
        part = dot_t(y_in[t], b_in[t])
        y_total = part if t == 0 else y_total + part
    last.wait()
    for h in range(2):
        cols = pl.ds(pl.multiple_of(idx[8 + h] * 256, 256), 256)
        half = slice(256 * h, 256 * h + 256)
        for i in range(4):
            rows = pl.ds(pl.multiple_of(idx[i], 128), 128)
            acc[rows, cols] = mine[rows, cols] - z_total[128 * i : 128 * i + 128, half]
            rows = pl.ds(pl.multiple_of(idx[i] + 128, 128), 128)
            if i < 3:
                acc[rows, cols] = mine[rows, cols] - y_total[128 * i : 128 * i + 128, half]
            else:
                acc[rows, cols] = mine[rows, cols]
    applied[...] = full_dot(acc[...], guess[...])


def late_kernel(
    idx, guess, zo, za, zb, ya, yb, bt, bb, ct, cb, acc, early,
    updated, applied, z_in, y_in, b_in, part, b_sems, sems,
):
    b_copies = columns_in(idx, (bt, bb, ct, cb), b_in, b_sems)
    z_copies = [
        pltpu.make_async_copy(zo, z_in.at[:128], sems.at[0]),
        pltpu.make_async_copy(za, z_in.at[128:320], sems.at[1]),
        pltpu.make_async_copy(zb, z_in.at[320:512], sems.at[5]),
        pltpu.make_async_copy(yb.at[128:], z_in.at[512:], sems.at[2]),
    ]
    y_copies = [
        pltpu.make_async_copy(ya, y_in.at[:256], sems.at[3]),
        pltpu.make_async_copy(yb.at[:128], y_in.at[256:], sems.at[4]),
    ]
    kept = [
        pltpu.make_async_copy(acc, updated, sems.at[6]),
        pltpu.make_async_copy(early, applied, sems.at[7]),
    ]
    started(b_copies[3] + z_copies + y_copies)
    for t in range(3):
        started(b_copies[t])
    started(kept)
    waited(b_copies[3] + z_copies)
    z = dot_t(z_in[...], b_in[3])
    waited(y_copies)
    y = z[512:]
    for t in range(3):
        waited(b_copies[t])
        y = y + dot_t(y_in[128 * t : 128 * t + 128, :], b_in[t])
    for h in range(2):
        cols = pl.ds(pl.multiple_of(idx[8 + h] * 256, 256), 256)
        half = slice(256 * h, 256 * h + 256)
        part[:512, cols] = z[:512, half]
        part[512:, cols] = y[:, half]
    last = full_dot(part[...], guess[...])
    waited(kept)
    for i in range(5):
        start = idx[i] if i < 4 else idx[3] + 128
        rows = pl.ds(pl.multiple_of(start, 128), 128)
        mine = slice(128 * i, 128 * i + 128)
        updated[rows, :] = updated[rows, :] - part[mine, :]
        applied[rows, :] = applied[rows, :] - last[mine]


def on_core(kernel, outs, inputs, flops, vmem_mib=24, scratch=(), whole=0):
    size = sum(a.size * a.dtype.itemsize for a in inputs)
    vmem = pl.BlockSpec(memory_space=pltpu.VMEM)
    smem = pl.BlockSpec(memory_space=pltpu.SMEM)
    away = pl.BlockSpec(memory_space=pltpu.HBM)
    return pl.pallas_call(
        kernel,
        out_shape=outs,
        in_specs=[smem] + [vmem] * (len(inputs) - 1 - whole) + [away] * whole,
        out_specs=jax.tree.map(lambda _: vmem, outs),
        scratch_shapes=list(scratch),
        cost_estimate=pl.CostEstimate(flops=flops, bytes_accessed=size, transcendentals=0),
        compiler_params=pltpu.CompilerParams(vmem_limit_bytes=vmem_mib * 1024 * 1024),
    )(*inputs)


def pack_kernel(own, prev, succ, far, out):
    for i, part in enumerate((own, prev, succ, far)):
        out[i] = part[...]


def pack(parts):
    vmem = pl.BlockSpec(memory_space=pltpu.VMEM)
    return pl.pallas_call(
        pack_kernel,
        out_shape=jax.ShapeDtypeStruct((4, *parts[0].shape), parts[0].dtype),
        in_specs=[vmem] * 4,
        out_specs=vmem,
        cost_estimate=pl.CostEstimate(flops=2**20, bytes_accessed=2**22, transcendentals=0),
        compiler_params=pltpu.CompilerParams(vmem_limit_bytes=8 * 1024 * 1024),
    )(*parts)


def gram_kernel(inverse, gram):
    keep = lax.broadcasted_iota(jnp.int32, (BS, BS), 0) >= lax.broadcasted_iota(jnp.int32, (BS, BS), 1)
    for i in range(2):
        g = jnp.where(keep, inverse[BS * i : BS * i + BS, :], 0.0)
        gram[i] = lax.dot_general(
            g, g, (((0,), (0,)), ((), ())), precision=lax.Precision.HIGHEST, preferred_element_type=F32
        )


def correct_kernel(gram, residual, correction, squares):
    for i in range(2):
        rows = slice(BS * i, BS * i + BS)
        correction[rows, :] = full_dot(gram[i], residual[rows, :])
    total = (residual[...] * residual[...]).reshape(128, 8, R).sum(axis=0)
    squares[...] = jnp.broadcast_to(total[None], (8, 8, R))


def body(trailing, panel, inverse_factor, block_inverse, guess, target):
    row_id = lax.axis_index("row")
    col_id = lax.axis_index("col")
    depth_id = lax.axis_index("depth")
    x_id, core_id = row_id // 2, row_id % 2
    starts = [256 * ((col_id + k) % 4) for k in (0, 3, 1, 2)]
    at = jnp.stack(starts + [depth_id * 1024, col_id * 1024]).astype(jnp.int32)
    top, bottom = factor_share(panel, inverse_factor, at)

    gram = pl.pallas_call(
        gram_kernel,
        out_shape=jax.ShapeDtypeStruct((2, BS, BS), F32),
        cost_estimate=pl.CostEstimate(flops=2**32, bytes_accessed=2**22, transcendentals=0),
        compiler_params=pltpu.CompilerParams(vmem_limit_bytes=16 * 1024 * 1024),
    )(block_inverse)

    b_own, b_other = [], []
    for half in (top, bottom):
        line = lax.ppermute(half, ALL, turned())
        parts = gather_direct(line, "row", 2, 8)
        packed = pack(parts)
        b_own.append(packed)
        b_other.append(lax.ppermute(packed, "row", [(i, i ^ 1) for i in range(8)]))

    z_parts = gather_direct(top, "col", 1, 4)
    y_all = joined(gather_direct(bottom, "depth", 1, 4))
    _, z_own_r, z_own_l, z_own_far = gather_direct(top, "depth", 1, 4)
    z_rest = joined(z_parts[1:])
    _, zr, zl, za, zb = gather_ring(z_rest, "depth", 1, 4)
    yd, yr, yl, ya, yb = gather_ring(y_all, "col", 1, 4)

    offsets = [256 * ((col_id + k) % 4) for k in (0, 3, 1, 2)]
    places = []
    for k in (0, 3, 1, 2):
        dx = (depth_id + k + 2 * (depth_id // 2) + col_id - x_id) % 4
        places.append(jnp.where(dx == 0, 0, jnp.where(dx == 3, 1, dx + 1)))
    idx = jnp.stack(offsets + places + [core_id, 1 - core_id, depth_id]).astype(jnp.int32)

    tile = jax.ShapeDtypeStruct((1024, 512), F32)
    narrow = jax.ShapeDtypeStruct((1024, R), F32)
    acc, early = on_core(
        early_kernel,
        (tile, narrow),
        (idx, guess, *z_parts, z_own_r, z_own_l, zr, zl, yd, yr, yl, *b_own, *b_other, trailing),
        2 * 512 * 1024 * (896 * 3 + 384),
        vmem_mib=60,
        scratch=(
            pltpu.VMEM((3, 512, 1024), BF16),
            pltpu.VMEM((4, 384, 1024), BF16),
            pltpu.VMEM((4, 512, 1024), BF16),
            pltpu.VMEM((1024, 512), F32),
            pltpu.SemaphoreType.DMA((16,)),
            pltpu.SemaphoreType.DMA((8,)),
            pltpu.SemaphoreType.DMA((12,)),
            pltpu.SemaphoreType.DMA,
        ),
        whole=16,
    )
    updated, applied = on_core(
        late_kernel,
        (tile, narrow),
        (idx, guess, z_own_far, za, zb, ya, yb, *b_own, *b_other, acc, early),
        2 * 512 * 1024 * 1024,
        vmem_mib=60,
        scratch=(
            pltpu.VMEM((640, 1024), BF16),
            pltpu.VMEM((384, 1024), BF16),
            pltpu.VMEM((4, 512, 1024), BF16),
            pltpu.VMEM((640, 512), F32),
            pltpu.SemaphoreType.DMA((16,)),
            pltpu.SemaphoreType.DMA((8,)),
        ),
        whole=11,
    )

    pieces = lax.all_to_all(applied.reshape(16, 64, R), PLANE, 0, 0, tiled=True)
    piece_id = col_id * 4 + depth_id
    part = lax.dynamic_slice_in_dim(target, piece_id * 64, 64, 0) - pieces.sum(axis=0)
    residual = lax.all_to_all(jnp.broadcast_to(part[None], (16, 64, R)), PLANE, 0, 0, tiled=True)
    residual = residual.reshape(1024, R)
    correction, squares = pl.pallas_call(
        correct_kernel,
        out_shape=(jax.ShapeDtypeStruct((1024, R), F32), jax.ShapeDtypeStruct((8, 8, R), F32)),
        cost_estimate=pl.CostEstimate(flops=2**30, bytes_accessed=2**22, transcendentals=0),
        compiler_params=pltpu.CompilerParams(vmem_limit_bytes=16 * 1024 * 1024),
    )(gram, residual)
    squares = lax.all_to_all(squares, "row", 0, 0, tiled=True).sum()
    residual_rms = jnp.sqrt(squares / (N * R))
    return (updated, correction, residual_rms.reshape(1))


def solution(mesh):
    placed = (
        P("row", "col"),
        P("row", "col"),
        P("depth", "col"),
        P("row", None),
        P(("col", "depth"), None),
        P("row", None),
    )
    return jax.shard_map(
        body,
        mesh=mesh,
        in_specs=placed,
        out_specs=(P("row", ("col", "depth")), P("row", None), P()),
        check_vma=False,
    )
```
